32 devices in a mesh: row: 4 (over x, core), col: 4 (over z), depth: 2 (over y).
Axes of the slice: x: 2, y: 2, z: 4, core: 2. Of those that a mesh axis runs over, the one named last changes fastest.
Arguments:
- tokens: bfloat16 [512, 4096], P(('col', 'depth'), 'row'), may hold values from -6 to 6
- w_gate: bfloat16 [4096, 14336], P('row', 'col'), may hold values from -0.09375 to 0.09375
- w_up: bfloat16 [4096, 14336], P('row', 'col'), may hold values from -0.09375 to 0.09375
- w_down: bfloat16 [14336, 4096], P('col', 'row'), may hold values from -0.046875 to 0.046875
- cotangent: bfloat16 [512, 4096], P(('col', 'depth'), 'row'), may hold values from -0.25 to 0.25
Outputs:
- mixed: bfloat16 [512, 4096], P(('col', 'depth'), 'row')
- grad_gate: bfloat16 [4096, 14336], P(('row', 'depth'), 'col')
- grad_up: bfloat16 [4096, 14336], P(('row', 'depth'), 'col')
- grad_down: bfloat16 [14336, 4096], P(('col', 'depth'), 'row')
The draws below stay inside these ranges and needn't reach their ends.
All inputs are finite; a program needn't handle non-finite values.
Results may differ from the reference program's by a relative error of at most 0.025.
Values may be sent and summed in bfloat16 or wider, within the bound.
A program may use at most 128 MiB of HBM per device.

```python
import jax
import jax.numpy as jnp
from jax import lax

D = 4096
FF = 14336
TOK_DEV = 64
TOKENS = 512
N_ROW = 4
N_COL = 4
N_DEPTH = 2


def steps_of(own_key, shape, pieces, low, top_value):
    level, own = 1.0, jax.random.fold_in(own_key, 6)
    for axis_at, parts in pieces:
        draws = jnp.exp(jax.random.uniform(jax.random.fold_in(own, axis_at), (parts,), jnp.float32, low / len(pieces), top_value / len(pieces)))
        level = level * jnp.repeat(draws, shape[axis_at] // parts).reshape([-1 if axis == axis_at else 1 for axis in range(len(shape))])
    return level


def noise(stream_key, shape, width, reach, split=(), kind=jnp.bfloat16):
    gain = steps_of(stream_key, shape, split, -0.22, 0.18) if split else 1.0
    values = jax.random.normal(stream_key, shape, jnp.float32) * width * gain
    return jnp.minimum(jnp.maximum(values, -reach), reach).astype(kind)


def setup_inputs(seed: int = 0) -> dict:
    splits = jax.random.split(jax.random.key(seed), 6)
    tokens = noise(splits[0], (TOKENS, D), 1.0, 6.0, ((0, 8), (1, 4)))
    w_gate = noise(splits[1], (D, FF), D ** -0.5, 0.09375, ((0, 4), (1, 4)))
    w_up = noise(splits[2], (D, FF), D ** -0.5, 0.09375, ((0, 4), (1, 4)))
    w_down = noise(splits[3], (FF, D), FF ** -0.5, 0.046875, ((0, 4), (1, 4)))
    cotangent = noise(splits[4], (TOKENS, D), (TOKENS ** -0.5), 0.25, ((0, 8), (1, 4)))
    return dict(tokens=tokens, w_gate=w_gate, w_up=w_up, w_down=w_down, cotangent=cotangent)


COLS_CONTRACT = (((1,), (1,)), ((), ()))
ROWS_CONTRACT = (((0,), (0,)), ((), ()))


def rounded_add(running, addend):
    rounded = lax.optimization_barrier(addend.astype(jnp.bfloat16))
    return running + rounded.astype(jnp.float32)


def layer_rows(array, layer_index):
    shaped = array.reshape(N_COL, N_DEPTH, TOK_DEV, array.shape[1])
    return shaped[:, layer_index].reshape(N_COL * TOK_DEV, array.shape[1])


def reference(tokens, w_gate, w_up, w_down, cotangent):
    feat_width = D // N_ROW
    token_count = tokens.shape[0]
    gate_sum = jnp.zeros((token_count, FF), jnp.float32)
    up_sum = jnp.zeros((token_count, FF), jnp.float32)
    hidden_grad = jnp.zeros((token_count, FF), jnp.float32)
    for block_index in range(N_ROW):
        lower_edge = block_index * feat_width
        upper_edge = lower_edge + feat_width
        tok_block = tokens[:, lower_edge:upper_edge]
        gate_sum = rounded_add(gate_sum, jnp.dot(tok_block, w_gate[lower_edge:upper_edge], preferred_element_type=jnp.float32))
        up_sum = rounded_add(up_sum, jnp.dot(tok_block, w_up[lower_edge:upper_edge], preferred_element_type=jnp.float32))
        hidden_grad = rounded_add(hidden_grad, lax.dot_general(cotangent[:, lower_edge:upper_edge], w_down[:, lower_edge:upper_edge], COLS_CONTRACT, preferred_element_type=jnp.float32))
    hidden = (jax.nn.silu(gate_sum) * up_sum).astype(jnp.bfloat16)
    mixed = jnp.dot(hidden, w_down, preferred_element_type=jnp.float32).astype(jnp.bfloat16)
    sigmoid_gate = jax.nn.sigmoid(gate_sum)
    d_gate = (hidden_grad * up_sum * sigmoid_gate * (1.0 + gate_sum * (1.0 - sigmoid_gate))).astype(jnp.bfloat16)
    d_up = (hidden_grad * gate_sum * sigmoid_gate).astype(jnp.bfloat16)
    grad_gate = jnp.zeros((D, FF), jnp.float32)
    grad_up = jnp.zeros((D, FF), jnp.float32)
    grad_down = jnp.zeros((FF, D), jnp.float32)
    for layer_index in range(N_DEPTH):
        tok_layer = layer_rows(tokens, layer_index)
        grad_gate = rounded_add(grad_gate, lax.dot_general(tok_layer, layer_rows(d_gate, layer_index), ROWS_CONTRACT, preferred_element_type=jnp.float32))
        grad_up = rounded_add(grad_up, lax.dot_general(tok_layer, layer_rows(d_up, layer_index), ROWS_CONTRACT, preferred_element_type=jnp.float32))
        grad_down = rounded_add(grad_down, lax.dot_general(layer_rows(hidden, layer_index), layer_rows(cotangent, layer_index), ROWS_CONTRACT, preferred_element_type=jnp.float32))
    return (mixed, grad_gate.astype(jnp.bfloat16), grad_up.astype(jnp.bfloat16), grad_down.astype(jnp.bfloat16))
```

```python
import functools

import jax
import jax.numpy as jnp
from jax import lax
from jax.sharding import PartitionSpec as P

COLS_CONTRACT = (((1,), (1,)), ((), ()))
ROWS_CONTRACT = (((0,), (0,)), ((), ()))


def gate_grads(hidden_grad, gate_sum, up_sum):
    sigmoid_gate = jax.nn.sigmoid(gate_sum)
    d_gate = (hidden_grad * up_sum * sigmoid_gate * (1.0 + gate_sum * (1.0 - sigmoid_gate))).astype(
        jnp.bfloat16
    )
    d_up = (hidden_grad * gate_sum * sigmoid_gate).astype(jnp.bfloat16)
    return (d_gate, d_up)


def layered_device(tokens, w_gate, w_up, w_down, cotangent):
    hid_width = w_gate.shape[1]
    token_rows = lax.all_gather(tokens, "col", axis=0, tiled=True)
    row_piece = token_rows
    joined = lax.psum_scatter(
        jnp.concatenate(
            [
                jnp.dot(row_piece, w_gate, preferred_element_type=jnp.float32),
                jnp.dot(row_piece, w_up, preferred_element_type=jnp.float32),
            ],
            axis=1,
        ).astype(jnp.bfloat16),
        "row",
        scatter_dimension=0,
        tiled=True,
    ).astype(jnp.float32)
    gate_sum = joined[:, :hid_width]
    up_sum = joined[:, hid_width:]
    hidden = (jax.nn.silu(gate_sum) * up_sum).astype(jnp.bfloat16)
    hidden_rows = lax.all_gather(hidden, "row", axis=0, tiled=True)
    row_piece = hidden_rows
    mixed = lax.psum_scatter(
        jnp.dot(row_piece, w_down, preferred_element_type=jnp.float32).astype(jnp.bfloat16),
        "col",
        scatter_dimension=0,
        tiled=True,
    )
    cot_rows = lax.all_gather(cotangent, "col", axis=0, tiled=True)
    row_piece = cot_rows
    hidden_grad = lax.psum_scatter(
        lax.dot_general(
            row_piece, w_down, COLS_CONTRACT, preferred_element_type=jnp.float32
        ).astype(jnp.bfloat16),
        "row",
        scatter_dimension=0,
        tiled=True,
    ).astype(jnp.float32)
    d_gate, d_up = gate_grads(hidden_grad, gate_sum, up_sum)
    d_gate_rows, d_up_rows = (
        lax.all_gather(d_gate, "row", axis=0, tiled=True),
        lax.all_gather(d_up, "row", axis=0, tiled=True),
    )
    down_term = lax.dot_general(
        hidden_rows, cot_rows, ROWS_CONTRACT, preferred_element_type=jnp.float32
    )
    grad_down = lax.psum_scatter(
        down_term.astype(jnp.bfloat16), "depth", scatter_dimension=0, tiled=True
    )
    layer_tokens = lax.all_to_all(token_rows, "depth", split_axis=1, concat_axis=0, tiled=True)
    block_rows = token_rows.shape[0]
    empty_grad = jnp.zeros((layer_tokens.shape[1], d_gate_rows.shape[1]), jnp.float32)
    first_row = jnp.int32(0)
    gate_total = empty_grad
    up_total = empty_grad
    gate_piece = lax.all_gather(d_gate_rows, "depth", axis=0, tiled=True)
    up_piece = lax.all_gather(d_up_rows, "depth", axis=0, tiled=True)
    for sub_index in range(gate_piece.shape[0] // block_rows):
        gate_block = gate_piece[sub_index * block_rows : (sub_index + 1) * block_rows]
        up_block = up_piece[sub_index * block_rows : (sub_index + 1) * block_rows]
        offset = first_row + sub_index * block_rows
        tok_block = lax.dynamic_slice_in_dim(layer_tokens, offset, block_rows, 0)
        gate_part = lax.optimization_barrier(
            lax.dot_general(
                tok_block, gate_block, ROWS_CONTRACT, preferred_element_type=jnp.float32
            ).astype(jnp.bfloat16)
        )
        up_part = lax.optimization_barrier(
            lax.dot_general(
                tok_block, up_block, ROWS_CONTRACT, preferred_element_type=jnp.float32
            ).astype(jnp.bfloat16)
        )
        gate_total = gate_total + gate_part.astype(jnp.float32)
        up_total = up_total + up_part.astype(jnp.float32)
    return (mixed, gate_total.astype(jnp.bfloat16), up_total.astype(jnp.bfloat16), grad_down)


def swap(x, axis, size, bit):
    return lax.ppermute(x, axis, [(i, i ^ bit) for i in range(size)])


def shift(x, size, step):
    return lax.ppermute(x, "col", [(i, (i + step) % size) for i in range(size)])


def gather_tokens(x, n_col):
    half = x.shape[0] // 2
    below = shift(x, n_col, 1)
    above = shift(x, n_col, -1)
    far = jnp.concatenate([shift(below[:half], n_col, 1), shift(above[half:], n_col, -1)], axis=0)
    other_x = swap(x, "depth", 2, 1)
    other_near = swap(jnp.concatenate([below, above], axis=0), "depth", 2, 1)
    other_far = swap(far, "depth", 2, 1)
    rows = x.shape[0]
    return jnp.concatenate(
        [x, below, far, above, other_x, other_near[:rows], other_far, other_near[rows:]], axis=0
    )


def relative(x, me, blocks):
    rows = x.shape[0] // blocks
    return jnp.concatenate(
        [lax.dynamic_slice_in_dim(x, (me ^ j) * rows, rows, 0) for j in range(blocks)], axis=0
    )


def f32(x):
    return x.astype(jnp.float32)


def bf16(x):
    return x.astype(jnp.bfloat16)


def row_sum_scatter(lhs, product, n_row):
    half = lhs.shape[0] // 2
    quarter = half // 2
    sent = swap(bf16(product(lhs[half:])), "row", n_row, 1)
    pair = product(lhs[:half]) + f32(sent)
    crossing = swap(bf16(pair[quarter:]), "row", n_row, 2)
    return pair[:quarter] + f32(crossing)


def row_gather(x, n_row):
    across = jnp.concatenate([x, swap(x, "row", n_row, 2)], axis=0)
    return jnp.concatenate([across, swap(across, "row", n_row, 1)], axis=0)


def grid_device(n_row, n_col, tokens, w_gate, w_up, w_down, cotangent):
    layer = lax.axis_index("depth")
    row = lax.axis_index("row")
    me = (row // 2) + 2 * (row % 2)
    width = w_gate.shape[1] // 2
    feats = w_gate.shape[0] // 2
    gate_w = lax.dynamic_slice_in_dim(w_gate, layer * width, width, 1)
    up_w = lax.dynamic_slice_in_dim(w_up, layer * width, width, 1)
    down_w = lax.dynamic_slice_in_dim(w_down, layer * width, width, 0)
    tok = relative(gather_tokens(tokens, n_col), me, n_row)
    cot = relative(gather_tokens(cotangent, n_col), me, n_row)

    gate_sum = row_sum_scatter(
        tok, lambda x: jnp.dot(x, gate_w, preferred_element_type=jnp.float32), n_row
    )
    up_sum = row_sum_scatter(
        tok, lambda x: jnp.dot(x, up_w, preferred_element_type=jnp.float32), n_row
    )
    hidden_grad = row_sum_scatter(
        cot,
        lambda x: lax.dot_general(x, down_w, COLS_CONTRACT, preferred_element_type=jnp.float32),
        n_row,
    )
    hidden = bf16(jax.nn.silu(gate_sum) * up_sum)
    d_gate, d_up = gate_grads(hidden_grad, gate_sum, up_sum)

    own = jnp.concatenate([d_gate, d_up], axis=1)
    part = own.shape[0] // 2
    near_x = swap(own, "row", n_row, 2)
    far_own = swap(own, "depth", 2, 1)
    far_x = jnp.concatenate(
        [swap(near_x[:part], "depth", 2, 1), swap(far_own[part:], "row", n_row, 2)], axis=0
    )
    near = jnp.concatenate([own, near_x], axis=0)
    near_core = swap(near, "row", n_row, 1)
    far_core = swap(far_own, "row", n_row, 1)
    far_x_core = swap(far_x, "row", n_row, 1)
    near_all = jnp.concatenate([near, near_core], axis=0)
    far_all = jnp.concatenate([far_core, far_x_core, far_own, far_x], axis=0)

    hidden_all = row_gather(hidden, n_row)
    mixed_part = relative(
        bf16(jnp.dot(hidden_all, down_w, preferred_element_type=jnp.float32)), me, n_row
    )
    layer_rows = mixed_part.shape[0] // 2
    layer_sum = bf16(f32(mixed_part[:layer_rows]) + f32(swap(mixed_part[layer_rows:], "depth", 2, 1)))
    rows = layer_rows // n_col
    mixed = f32(layer_sum[:rows])
    for step in range(1, n_col):
        mixed = mixed + f32(shift(layer_sum[step * rows : (step + 1) * rows], n_col, -step))
    mixed = bf16(mixed)

    grad_down = bf16(
        lax.dot_general(hidden_all, cot, ROWS_CONTRACT, preferred_element_type=jnp.float32)
    )
    tok_feats = lax.dynamic_slice_in_dim(tok, layer * feats, feats, 1)

    def weight_grad(d_rows):
        return bf16(
            lax.dot_general(tok_feats, d_rows, ROWS_CONTRACT, preferred_element_type=jnp.float32)
        )

    first = layer == 0

    def place(near_half, far_half):
        return jnp.where(
            first,
            jnp.concatenate([near_half, far_half], axis=1),
            jnp.concatenate([far_half, near_half], axis=1),
        )

    grad_gate = place(weight_grad(near_all[:, :width]), weight_grad(far_all[:, :width]))
    grad_up = place(weight_grad(near_all[:, width:]), weight_grad(far_all[:, width:]))
    return (mixed, grad_gate, grad_up, grad_down)


def solution(mesh):
    placed = (
        P(("col", "depth"), "row"),
        P("row", "col"),
        P("row", "col"),
        P("col", "row"),
        P(("col", "depth"), "row"),
    )
    n_row, n_col = mesh.shape["row"], mesh.shape["col"]
    if (n_row, n_col, mesh.shape["depth"]) == (4, 4, 2):
        per_device = functools.partial(grid_device, n_row, n_col)
    else:
        per_device = layered_device
    return jax.shard_map(
        per_device,
        mesh=mesh,
        in_specs=placed,
        out_specs=(
            P(("col", "depth"), "row"),
            P(("row", "depth"), "col"),
            P(("row", "depth"), "col"),
            P(("col", "depth"), "row"),
        ),
        check_vma=False,
    )
```

```python
import functools

import jax
import jax.numpy as jnp
from jax import lax
from jax.sharding import PartitionSpec as P

COLS_CONTRACT = (((1,), (1,)), ((), ()))
ROWS_CONTRACT = (((0,), (0,)), ((), ()))


def gate_grads(hidden_grad, gate_sum, up_sum):
    sigmoid_gate = jax.nn.sigmoid(gate_sum)
    d_gate = (hidden_grad * up_sum * sigmoid_gate * (1.0 + gate_sum * (1.0 - sigmoid_gate))).astype(
        jnp.bfloat16
    )
    d_up = (hidden_grad * gate_sum * sigmoid_gate).astype(jnp.bfloat16)
    return (d_gate, d_up)


def layered_device(tokens, w_gate, w_up, w_down, cotangent):
    hid_width = w_gate.shape[1]
    token_rows = lax.all_gather(tokens, "col", axis=0, tiled=True)
    row_piece = token_rows
    joined = lax.psum_scatter(
        jnp.concatenate(
            [
                jnp.dot(row_piece, w_gate, preferred_element_type=jnp.float32),
                jnp.dot(row_piece, w_up, preferred_element_type=jnp.float32),
            ],
            axis=1,
        ).astype(jnp.bfloat16),
        "row",
        scatter_dimension=0,
        tiled=True,
    ).astype(jnp.float32)
    gate_sum = joined[:, :hid_width]
    up_sum = joined[:, hid_width:]
    hidden = (jax.nn.silu(gate_sum) * up_sum).astype(jnp.bfloat16)
    hidden_rows = lax.all_gather(hidden, "row", axis=0, tiled=True)
    row_piece = hidden_rows
    mixed = lax.psum_scatter(
        jnp.dot(row_piece, w_down, preferred_element_type=jnp.float32).astype(jnp.bfloat16),
        "col",
        scatter_dimension=0,
        tiled=True,
    )
    cot_rows = lax.all_gather(cotangent, "col", axis=0, tiled=True)
    row_piece = cot_rows
    hidden_grad = lax.psum_scatter(
        lax.dot_general(
            row_piece, w_down, COLS_CONTRACT, preferred_element_type=jnp.float32
        ).astype(jnp.bfloat16),
        "row",
        scatter_dimension=0,
        tiled=True,
    ).astype(jnp.float32)
    d_gate, d_up = gate_grads(hidden_grad, gate_sum, up_sum)
    d_gate_rows, d_up_rows = (
        lax.all_gather(d_gate, "row", axis=0, tiled=True),
        lax.all_gather(d_up, "row", axis=0, tiled=True),
    )
    down_term = lax.dot_general(
        hidden_rows, cot_rows, ROWS_CONTRACT, preferred_element_type=jnp.float32
    )
    grad_down = lax.psum_scatter(
        down_term.astype(jnp.bfloat16), "depth", scatter_dimension=0, tiled=True
    )
    layer_tokens = lax.all_to_all(token_rows, "depth", split_axis=1, concat_axis=0, tiled=True)
    block_rows = token_rows.shape[0]
    empty_grad = jnp.zeros((layer_tokens.shape[1], d_gate_rows.shape[1]), jnp.float32)
    first_row = jnp.int32(0)
    gate_total = empty_grad
    up_total = empty_grad
    gate_piece = lax.all_gather(d_gate_rows, "depth", axis=0, tiled=True)
    up_piece = lax.all_gather(d_up_rows, "depth", axis=0, tiled=True)
    for sub_index in range(gate_piece.shape[0] // block_rows):
        gate_block = gate_piece[sub_index * block_rows : (sub_index + 1) * block_rows]
        up_block = up_piece[sub_index * block_rows : (sub_index + 1) * block_rows]
        offset = first_row + sub_index * block_rows
        tok_block = lax.dynamic_slice_in_dim(layer_tokens, offset, block_rows, 0)
        gate_part = lax.optimization_barrier(
            lax.dot_general(
                tok_block, gate_block, ROWS_CONTRACT, preferred_element_type=jnp.float32
            ).astype(jnp.bfloat16)
        )
        up_part = lax.optimization_barrier(
            lax.dot_general(
                tok_block, up_block, ROWS_CONTRACT, preferred_element_type=jnp.float32
            ).astype(jnp.bfloat16)
        )
        gate_total = gate_total + gate_part.astype(jnp.float32)
        up_total = up_total + up_part.astype(jnp.float32)
    return (mixed, gate_total.astype(jnp.bfloat16), up_total.astype(jnp.bfloat16), grad_down)


def swap(x, axis, size, bit):
    return lax.ppermute(x, axis, [(i, i ^ bit) for i in range(size)])


def shift(x, size, step):
    return lax.ppermute(x, "col", [(i, (i + step) % size) for i in range(size)])


def gather_tokens(x, n_col):
    half = x.shape[0] // 2
    below = shift(x, n_col, 1)
    above = shift(x, n_col, -1)
    far = jnp.concatenate([shift(below[:half], n_col, 1), shift(above[half:], n_col, -1)], axis=0)
    other_x = swap(x, "depth", 2, 1)
    other_near = swap(jnp.concatenate([below, above], axis=0), "depth", 2, 1)
    other_far = swap(far, "depth", 2, 1)
    rows = x.shape[0]
    return jnp.concatenate(
        [x, below, far, above, other_x, other_near[:rows], other_far, other_near[rows:]], axis=0
    )


def relative(x, me, blocks):
    rows = x.shape[0] // blocks
    return jnp.concatenate(
        [lax.dynamic_slice_in_dim(x, (me ^ j) * rows, rows, 0) for j in range(blocks)], axis=0
    )


def f32(x):
    return x.astype(jnp.float32)


def bf16(x):
    return x.astype(jnp.bfloat16)


def row_sum_scatter(lhs, product, n_row):
    half = lhs.shape[0] // 2
    quarter = half // 2
    sent = swap(bf16(product(lhs[half:])), "row", n_row, 1)
    pair = product(lhs[:half]) + f32(sent)
    crossing = swap(bf16(pair[quarter:]), "row", n_row, 2)
    return pair[:quarter] + f32(crossing)


def row_gather(x, n_row):
    across = jnp.concatenate([x, swap(x, "row", n_row, 2)], axis=0)
    return jnp.concatenate([across, swap(across, "row", n_row, 1)], axis=0)


def grid_device(n_row, n_col, tokens, w_gate, w_up, w_down, cotangent):
    layer = lax.axis_index("depth")
    row = lax.axis_index("row")
    me = (row // 2) + 2 * (row % 2)
    width = w_gate.shape[1] // 2
    feats = w_gate.shape[0] // 2
    gate_w = lax.dynamic_slice_in_dim(w_gate, layer * width, width, 1)
    up_w = lax.dynamic_slice_in_dim(w_up, layer * width, width, 1)
    down_w = lax.dynamic_slice_in_dim(w_down, layer * width, width, 0)
    tok = relative(gather_tokens(tokens, n_col), me, n_row)
    cot = relative(gather_tokens(cotangent, n_col), me, n_row)

    gate_sum = row_sum_scatter(
        tok, lambda x: jnp.dot(x, gate_w, preferred_element_type=jnp.float32), n_row
    )
    up_sum = row_sum_scatter(
        tok, lambda x: jnp.dot(x, up_w, preferred_element_type=jnp.float32), n_row
    )
    hidden_grad = row_sum_scatter(
        cot,
        lambda x: lax.dot_general(x, down_w, COLS_CONTRACT, preferred_element_type=jnp.float32),
        n_row,
    )
    hidden = bf16(jax.nn.silu(gate_sum) * up_sum)
    d_gate, d_up = gate_grads(hidden_grad, gate_sum, up_sum)

    own = jnp.concatenate([d_gate, d_up], axis=1)
    part = own.shape[0] // 2
    near_x = swap(own, "row", n_row, 2)
    far_own = swap(own, "depth", 2, 1)
    far_x = jnp.concatenate(
        [swap(near_x[:part], "depth", 2, 1), swap(far_own[part:], "row", n_row, 2)], axis=0
    )
    near = jnp.concatenate([own, near_x], axis=0)
    near_core = swap(near, "row", n_row, 1)
    far_core = swap(far_own, "row", n_row, 1)
    far_x_core = swap(far_x, "row", n_row, 1)
    near_all = jnp.concatenate([near, near_core], axis=0)
    far_all = jnp.concatenate([far_core, far_x_core, far_own, far_x], axis=0)

    hidden_all = row_gather(hidden, n_row)
    mixed_part = relative(
        bf16(jnp.dot(hidden_all, down_w, preferred_element_type=jnp.float32)), me, n_row
    )
    layer_rows = mixed_part.shape[0] // 2
    layer_sum = bf16(f32(mixed_part[:layer_rows]) + f32(swap(mixed_part[layer_rows:], "depth", 2, 1)))
    rows = layer_rows // n_col
    arrived = [
        shift(layer_sum[step * rows : (step + 1) * rows], n_col, -step) for step in range(1, n_col)
    ]

    grad_down = bf16(
        lax.dot_general(hidden_all, cot, ROWS_CONTRACT, preferred_element_type=jnp.float32)
    )
    tok_feats = lax.dynamic_slice_in_dim(tok, layer * feats, feats, 1)

    def weight_grad(d_rows):
        return bf16(
            lax.dot_general(tok_feats, d_rows, ROWS_CONTRACT, preferred_element_type=jnp.float32)
        )

    first = layer == 0

    def place(near_half, far_half):
        return jnp.where(
            first,
            jnp.concatenate([near_half, far_half], axis=1),
            jnp.concatenate([far_half, near_half], axis=1),
        )

    grad_gate = weight_grad(place(near_all[:, :width], far_all[:, :width]))
    grad_up = weight_grad(place(near_all[:, width:], far_all[:, width:]))
    grad_gate, grad_up, arrived = lax.optimization_barrier((grad_gate, grad_up, arrived))
    mixed = f32(layer_sum[:rows])
    for share in arrived:
        mixed = mixed + f32(share)
    mixed = bf16(mixed)
    return (mixed, grad_gate, grad_up, grad_down)


def solution(mesh):
    placed = (
        P(("col", "depth"), "row"),
        P("row", "col"),
        P("row", "col"),
        P("col", "row"),
        P(("col", "depth"), "row"),
    )
    n_row, n_col = mesh.shape["row"], mesh.shape["col"]
    if (n_row, n_col, mesh.shape["depth"]) == (4, 4, 2):
        per_device = functools.partial(grid_device, n_row, n_col)
    else:
        per_device = layered_device
    return jax.shard_map(
        per_device,
        mesh=mesh,
        in_specs=placed,
        out_specs=(
            P(("col", "depth"), "row"),
            P(("row", "depth"), "col"),
            P(("row", "depth"), "col"),
            P(("col", "depth"), "row"),
        ),
        check_vma=False,
    )
```
